1024 devices in a mesh: lon: 32 (over y, x, core), lat: 32 (over z).
Axes of the slice: x: 4, y: 4, z: 32, core: 2. Of those that a mesh axis runs over, the one named last changes fastest.
Arguments:
- increment: float32 [2, 137, 256, 4096], P(None, None, 'lat', 'lon'), may hold values from -6 to 6
- mixing: float32 [2, 137], replicated, may hold values from 0.02 to 0.12
- mixing_mask: int32 [256, 4096], P('lat', 'lon'), may hold values 0 or 1
- jacobian: bfloat16 [40, 20, 274], replicated, may hold values from -0.375 to 0.375
- fp_col: int32 [32, 32, 256], P('lon', 'lat'), may hold values from -1 to 1023, as said below
- fp_class: int32 [32, 32, 256], P('lon', 'lat'), may hold values from -1 to 39, as said below
- obs: float32 [32, 32, 20, 256], P('lon', 'lat'), may hold values from -6 to 6
- obs_weight: float32 [32, 32, 20, 256], P('lon', 'lat'), may hold values from 0.25 to 4
Outputs:
- gradient: float32 [2, 137, 256, 4096], P(None, None, 'lat', 'lon')
The draws below stay inside these ranges and needn't reach their ends.
Inputs may be any that keep to these rules, and one draw needn't show every extreme that they name: `fp_col`: -1 marks an empty slot; in each group of 8 slots from one tile to one owner the live slots come first; only owners with lat index a multiple of 8 have live slots; in every draw some group is full, and some owner is full from every source tile. `fp_class`: entry [l, d, s * 8 + k] is the class of the footprint in slot [l, s, d * 8 + k] of fp_col, and -1 exactly where that slot is empty.
All inputs are finite; a program needn't handle non-finite values. No bound on the sum of `mixing_mask` on one device may be relied on, other than what follows from the above.
Results may differ from the reference program's by a relative error of at most 0.00031.
Values may be sent and summed in bfloat16 or wider, within the bound.
No kernel may reach another device: no remote copies, remote signals or barrier semaphores. Data moves between devices by JAX's collectives and lax.ppermute only.
A program may use at most 32 MiB of HBM per device.

```python
import math
import jax
import jax.numpy as jnp
from jax import lax

LEV = 137
CH = 20
NCLS = 40
CLAT = 8
CLON = 128
SLOT = 8
LEV2 = 274
COLS = 1024
TILES_LON = 32
TILES_LAT = 32
OWN_EVERY = 8
NLAT = 256
NLON = 4096


def slot_layout(key):
    base = jax.random.fold_in(key, 7001)
    key_count, key_src, key_dest, key_col, key_class = jax.random.split(base, 5)
    shape = (TILES_LON, TILES_LAT, TILES_LAT)
    counts = jax.random.randint(key_count, shape, max(1, SLOT // 3), SLOT + 1)
    full_src = jax.random.randint(key_src, (TILES_LON,), 0, TILES_LAT)
    full_dest = jax.random.randint(key_dest, (TILES_LON,), 0, TILES_LAT // OWN_EVERY) * OWN_EVERY
    index_src = jnp.arange(TILES_LAT)
    counts = jnp.where(index_src[None, :, None] == full_src[:, None, None], SLOT, counts)
    counts = jnp.where(index_src[None, None, :] == full_dest[:, None, None], SLOT, counts)
    counts = jnp.where((index_src % OWN_EVERY == 0)[None, None, :], counts, 0)
    is_live = jnp.arange(SLOT)[None, None, None, :] < counts[..., None]
    columns = jax.random.randint(key_col, shape + (SLOT,), 0, COLS)
    classes = jax.random.randint(key_class, shape + (SLOT,), 0, NCLS)
    return (is_live, columns, classes)


def draw_fp_col(key, part):
    is_live, columns, classes = slot_layout(key)
    picked = jnp.where(is_live, columns, -1)
    return picked.reshape(TILES_LON, TILES_LAT, TILES_LAT * SLOT).astype(jnp.int32)


def draw_fp_class(key, part):
    is_live, columns, classes = slot_layout(key)
    picked = jnp.where(is_live, classes, -1).transpose(0, 2, 1, 3)
    return picked.reshape(TILES_LON, TILES_LAT, TILES_LAT * SLOT).astype(jnp.int32)


def set_ends(result, rng, low, largest):
    extent = result.shape
    place = [jax.random.randint(jax.random.fold_in(rng, axis), (), 0, extent[axis]) for axis in range(len(extent))]
    result = result.at[tuple(place)].set(low)
    longest = extent.index(max(extent))
    place[longest] = (place[longest] + 1) % extent[longest]
    return result.at[tuple(place)].set(largest)


def block_scale(stream_key, dims, pieces, low, high):
    loudness = 1.0
    for dim, parts in pieces:
        steps = jax.random.uniform(jax.random.fold_in(jax.random.fold_in(stream_key, 6), dim), (parts,), jnp.float32, low / len(pieces), high / len(pieces))
        loudness = loudness * jnp.repeat(jnp.exp(steps), dims[dim] // parts).reshape((-1,) + (1,) * (len(dims) - 1 - dim))
    return loudness


def normal_values(key, shape, deviation, bound, cuts=(), held_as=jnp.bfloat16):
    factor_of = block_scale(key, shape, cuts, -0.22, 0.18) if cuts else 1.0
    array = jax.random.normal(key, shape, jnp.float32) * deviation * factor_of
    return jnp.minimum(jnp.maximum(array, -bound), bound).astype(held_as)


def setup_inputs(seed: int = 0) -> dict:
    key_of = jax.random.split(jax.random.key(seed), 9)
    increment = normal_values(key_of[0], (2, LEV, NLAT, NLON), 1.0, 6.0, ((2, 32), (3, 32)), jnp.float32)
    mixing = jnp.clip(jnp.exp(jax.random.uniform(key_of[1], (2, LEV), jnp.float32, math.log(0.02), math.log(0.12))), 0.02, 0.12)
    mixing_mask = set_ends((jax.random.randint(key_of[2], (NLAT, NLON), 0, 4) < 3).astype(jnp.int32), jax.random.fold_in(key_of[2], 1), 0, 1)
    jacobian = normal_values(key_of[3], (NCLS, CH, LEV2), LEV2 ** -0.5, 0.375)
    fp_col = draw_fp_col(jax.random.fold_in(key_of[8], 71), 0)
    fp_class = draw_fp_class(jax.random.fold_in(key_of[8], 71), 0)
    obs = normal_values(key_of[6], (TILES_LON, TILES_LAT, CH, TILES_LAT * SLOT), 1.0, 6.0, ((0, 32), (1, 32)), jnp.float32)
    obs_weight = jnp.clip(jnp.exp(math.log(4.0) - 2.7725887 * jax.random.uniform(key_of[7], (TILES_LON, TILES_LAT, CH, TILES_LAT * SLOT), jnp.float32) ** block_scale(key_of[7], (TILES_LON, TILES_LAT, CH, TILES_LAT * SLOT), ((0, 32), (1, 32)), -0.2, 0.2)), 0.25, 4.0)
    return dict(increment=increment, mixing=mixing, mixing_mask=mixing_mask, jacobian=jacobian, fp_col=fp_col, fp_class=fp_class, obs=obs, obs_weight=obs_weight)


def laplace(field):
    across = jnp.roll(field, 1, 3) + jnp.roll(field, -1, 3)
    padded = jnp.pad(field, ((0, 0), (0, 0), (1, 1), (0, 0)))
    return across + padded[:, :, 2:] + padded[:, :, :-2] - 4.0 * field


def reference(increment, mixing, mixing_mask, jacobian, fp_col, fp_class, obs, obs_weight):
    mix_scale = mixing[:, :, None, None] * mixing_mask.astype(jnp.float32)[None, None]
    advanced = increment + mix_scale * laplace(increment)
    state_bf = advanced.astype(jnp.bfloat16)
    tile_cols = state_bf.reshape(LEV2, TILES_LAT, CLAT, TILES_LON, CLON).transpose(3, 1, 0, 2, 4)
    tile_cols = tile_cols.reshape(TILES_LON * TILES_LAT, LEV2, COLS)
    slots = TILES_LAT * SLOT
    src_cols = fp_col.reshape(TILES_LON * TILES_LAT, slots)
    src_class = fp_class.reshape(TILES_LON, TILES_LAT, TILES_LAT, SLOT).transpose(0, 2, 1, 3)
    src_class = src_class.reshape(TILES_LON * TILES_LAT, slots)
    src_obs = obs.reshape(TILES_LON, TILES_LAT, CH, TILES_LAT, SLOT).transpose(0, 3, 2, 1, 4)
    src_obs = src_obs.reshape(TILES_LON * TILES_LAT, CH, slots)
    src_weight = obs_weight.reshape(TILES_LON, TILES_LAT, CH, TILES_LAT, SLOT).transpose(0, 3, 2, 1, 4)
    src_weight = src_weight.reshape(TILES_LON * TILES_LAT, CH, slots)

    def per_block(items):
        tile, wanted, classes, observed, weights = items
        is_live = wanted >= 0
        safe_col = jnp.maximum(wanted, 0).astype(jnp.int32)
        picked = jnp.take(tile, safe_col, axis=1).astype(jnp.float32) * is_live.astype(jnp.float32)[None]
        chosen = jacobian[jnp.maximum(classes, 0).astype(jnp.int32)].astype(jnp.float32)
        evolved = jnp.einsum("sck,ks->cs", chosen, picked)
        weighted = jnp.where(is_live[None], weights * (evolved - observed), 0.0).astype(jnp.bfloat16)
        adj_col = jnp.einsum("sck,cs->ks", chosen, weighted.astype(jnp.float32))
        return jnp.zeros((LEV2, COLS), jnp.float32).at[:, safe_col].add(adj_col)

    summed = lax.map(per_block, (tile_cols, src_cols, src_class, src_obs, src_weight))
    summed = summed.reshape(TILES_LON, TILES_LAT, LEV2, CLAT, CLON).transpose(2, 1, 3, 0, 4)
    summed = summed.reshape(2, LEV, NLAT, NLON)
    return increment + summed + laplace(mix_scale * summed)
```

```python
import jax
import jax.numpy as jnp
from jax import lax
from jax.experimental import pallas as pl
from jax.experimental.pallas import tpu as pltpu
from jax.sharding import PartitionSpec as P

OWN_EVERY = 8
SLOT = 8
ROWS = 8
LANES = 128
STRIDE = 48
CH = 20
NOWHERE = -1000000


def iota(shape, dim):
    return lax.broadcasted_iota(jnp.int32, shape, dim)


def call(body, out_shape, scratch=(), flops=1000000):
    return pl.pallas_call(
        body,
        out_shape=out_shape,
        scratch_shapes=list(scratch),
        cost_estimate=pl.CostEstimate(flops=flops, bytes_accessed=1000000, transcendentals=0),
    )


def record_spots():
    return [((k * STRIDE) // LANES, (k * STRIDE) % LANES) for k in range(SLOT)]


def records_body(obs_ref, weight_ref, class_ref, out_ref, wide_ref, tall_ref, flat_ref):
    peers = out_ref.shape[0]
    wide_ref[...] = jnp.zeros(wide_ref.shape, jnp.float32)
    for ch in range(CH):
        wide_ref[ch : ch + 1, :] = obs_ref[ch]
        wide_ref[24 + ch : 25 + ch, :] = weight_ref[ch]
    wide_ref[CH : CH + 1, :] = class_ref[0].astype(jnp.float32)
    tall_ref[...] = jnp.transpose(wide_ref[...])
    lane = iota((peers, LANES), 1)
    tiles = [jnp.zeros((peers, LANES), jnp.float32) for _ in range(SLOT * STRIDE // LANES)]
    for k, (tile, off) in enumerate(record_spots()):
        part = tall_ref[pl.ds(k, peers, stride=SLOT), :]
        part = pltpu.roll(part, off, 1) if off else part
        if off + STRIDE <= LANES:
            tiles[tile] = tiles[tile] + part
        else:
            tiles[tile] = tiles[tile] + jnp.where(lane >= off, part, 0.0)
            tiles[tile + 1] = tiles[tile + 1] + jnp.where(lane < off, part, 0.0)
    for i, value in enumerate(tiles):
        flat_ref[:, i * LANES : (i + 1) * LANES] = value
    for s in range(peers):
        out_ref[s] = flat_ref[s : s + 1, :]


def edges_body(inc_ref, first_ref, last_ref, right_ref, left_ref):
    depth = first_ref.shape[0]
    lane = iota((depth, LANES), 1)
    right = jnp.zeros((depth, LANES), jnp.float32)
    left = jnp.zeros((depth, LANES), jnp.float32)
    for r in range(ROWS):
        row = inc_ref[pl.ds(r, depth, stride=ROWS), :]
        if r == 0:
            first_ref[...] = row
        if r == ROWS - 1:
            last_ref[...] = row
        right = jnp.where(lane == r, pltpu.roll(row, r + 1, 1), right)
        left = jnp.where(lane == ROWS + r, pltpu.roll(row, ROWS + r, 1), left)
    right_ref[...] = right
    left_ref[...] = left


def state_body(inc_ref, up_ref, down_ref, from_left_ref, from_right_ref, col_ref, mask_ref,
               mix_ref, jac_ref, seen_ref, meta_ref):
    depth = up_ref.shape[0]
    lane8 = iota((8, LANES), 1)
    cols = jnp.full((8, LANES), NOWHERE, jnp.int32)
    owners = col_ref.shape[1] // (SLOT * OWN_EVERY)
    for g in range(owners):
        start = g * SLOT * OWN_EVERY
        tile = jnp.broadcast_to(col_ref[:, start // LANES * LANES : start // LANES * LANES + LANES], (8, LANES))
        shift = (g * SLOT - start % LANES) % LANES
        tile = pltpu.roll(tile, shift, 1) if shift else tile
        cols = jnp.where((lane8 >= g * SLOT) & (lane8 < (g + 1) * SLOT), tile, cols)
    cols = jnp.where(cols >= 0, cols, NOWHERE)
    both = jnp.where(lane8 < 32, cols, jnp.where(lane8 < 64, pltpu.roll(cols, 32, 1), NOWHERE))
    want = jnp.broadcast_to(both[0:1, :], (LANES, LANES))
    sub = iota((LANES, LANES), 0)
    plain = iota((LANES, LANES), 1) < 32

    def split_dot(x, chosen):
        high = x.astype(jnp.bfloat16)
        low = (x - high.astype(jnp.float32)).astype(jnp.bfloat16)
        return jnp.dot(
            jnp.concatenate([high, low], 1), jnp.concatenate([chosen, chosen], 0),
            preferred_element_type=jnp.float32,
        )

    total = jnp.zeros((depth, LANES), jnp.float32)
    masked = jnp.zeros((8, LANES), jnp.float32)
    for r in range(ROWS):
        point = sub + r * LANES
        here = jnp.where(want == point, 1.0, 0.0)
        beside = jnp.where((want == point - 1) & (sub != 0), 1.0, 0.0)
        beside = beside + jnp.where((want == point + 1) & (sub != LANES - 1), 1.0, 0.0)
        beside = beside + jnp.where((want == point - LANES) | (want == point + LANES), 1.0, 0.0)
        chosen = jnp.where(plain, here, beside - 4.0 * here).astype(jnp.bfloat16)
        total = total + split_dot(inc_ref[pl.ds(r, depth, stride=ROWS), :], chosen)
        mask_row = jnp.broadcast_to(mask_ref[r : r + 1, :].astype(jnp.bfloat16), (8, LANES))
        masked = masked + jnp.dot(mask_row, chosen, preferred_element_type=jnp.float32)
    near = ~plain
    chosen = jnp.where(near & (want == sub), 1.0, 0.0).astype(jnp.bfloat16)
    total = total + split_dot(up_ref[...], chosen)
    chosen = jnp.where(near & (want == sub + (ROWS - 1) * LANES), 1.0, 0.0).astype(jnp.bfloat16)
    total = total + split_dot(down_ref[...], chosen)
    on_left = (sub < ROWS) & (want == sub * LANES)
    on_right = (sub >= ROWS) & (sub < 2 * ROWS) & (want == (sub - ROWS) * LANES + LANES - 1)
    chosen = jnp.where(near & (on_left | on_right), 1.0, 0.0).astype(jnp.bfloat16)
    total = total + split_dot(from_left_ref[...] + from_right_ref[...], chosen)

    state = total + mix_ref[...] * masked[0:1, :] * pltpu.roll(total, LANES - 32, 1)
    state = jnp.where(iota((depth, LANES), 1) < 32, state, 0.0).astype(jnp.bfloat16)
    seen_ref[...] = jnp.dot(jac_ref[...], state, preferred_element_type=jnp.float32)
    meta_ref[0:1, :] = cols[0:1, :].astype(jnp.float32)
    meta_ref[1:2, :] = masked[0:1, :]
    meta_ref[2:8, :] = jnp.zeros((6, LANES), jnp.float32)


def departures_body(records_ref, seen_ref, meta_ref, out_ref, row_ref, spot_ref):
    owners = records_ref.shape[0] // OWN_EVERY
    classes = seen_ref.shape[0] // CH
    row_ref[...] = jnp.zeros(row_ref.shape, jnp.float32)
    spot_ref[...] = jnp.zeros(spot_ref.shape, jnp.float32)
    for g in range(owners):
        row_ref[g : g + 1, :] = records_ref[g * OWN_EVERY]
    lane8 = iota((8, LANES), 1)
    tiles = [row_ref[:, i * LANES : (i + 1) * LANES] for i in range(SLOT * STRIDE // LANES)]
    for k, (tile, off) in enumerate(record_spots()):
        part = pltpu.roll(tiles[tile], LANES - off, 1) if off else tiles[tile]
        if off + STRIDE > LANES:
            part = jnp.where(lane8 < LANES - off, part, pltpu.roll(tiles[tile + 1], LANES - off, 1))
        for g in range(owners):
            spot_ref[g * SLOT + k : g * SLOT + k + 1, :] = part[g : g + 1, :]
    turned = jnp.transpose(spot_ref[...])
    lane1 = iota((1, LANES), 1)
    kind = jnp.where(lane1 < owners * SLOT, turned[CH : CH + 1, :], -1.0)
    chosen = jnp.broadcast_to(kind, (classes, LANES)).astype(jnp.int32) == iota((classes, LANES), 0)
    out_ref[...] = jnp.zeros(out_ref.shape, jnp.float32)
    for ch in range(CH):
        rows = seen_ref[ch * classes : (ch + 1) * classes, :]
        out_ref[ch : ch + 1, :] = jnp.sum(jnp.where(chosen, rows, 0.0), axis=0, keepdims=True)
    evolved = out_ref[0:CH, :]
    weighted = turned[24 : 24 + CH, :] * (evolved - turned[0:CH, :])
    weighted = jnp.where(jnp.broadcast_to(kind, (CH, LANES)) >= 0, weighted, 0.0)
    out_ref[0:CH, :] = weighted.astype(jnp.bfloat16).astype(jnp.float32)
    live = lane1 < owners * SLOT
    out_ref[CH : CH + 1, :] = jnp.where(live, kind, 0.0)
    out_ref[CH + 1 : CH + 2, :] = jnp.where(live, meta_ref[0:1, :], 0.0)
    out_ref[CH + 2 : CH + 3, :] = jnp.where(live, meta_ref[1:2, :], 0.0)


def gradient_body(own_ref, left_ref, right_ref, up_ref, down_ref, turned_jac_ref, mix_ref, inc_ref,
                  out_ref, spread_ref, flip_ref):
    depth = turned_jac_ref.shape[0]
    classes = turned_jac_ref.shape[1] // CH
    four = own_ref[...] + pltpu.roll(left_ref[...], 32, 1) + pltpu.roll(right_ref[...], 64, 1)
    four = four + pltpu.roll(up_ref[...], 96, 1)
    both = jnp.concatenate([four, down_ref[...]], 1)
    kinds = jnp.broadcast_to(both[CH : CH + 1, :], (classes, 2 * LANES)).astype(jnp.int32)
    chosen = kinds == iota((classes, 2 * LANES), 0)
    for ch in range(CH):
        spread_ref[ch * classes : (ch + 1) * classes, :] = jnp.where(chosen, both[ch : ch + 1, :], 0.0)
    adjoint = jnp.dot(turned_jac_ref[...], spread_ref[...].astype(jnp.bfloat16), preferred_element_type=jnp.float32)

    lane = iota((depth, LANES), 1)
    own = jnp.where(lane < 32, adjoint[:, 0:LANES], 0.0)
    own_high = own.astype(jnp.bfloat16).astype(jnp.float32)
    rest = own - own_high
    own_mid = rest.astype(jnp.bfloat16).astype(jnp.float32)
    own_low = rest - own_mid
    summed = own_high + pltpu.roll(own_mid, 32, 1) + pltpu.roll(own_low, 64, 1)
    mixed = mix_ref[...] * adjoint
    mixed_high = mixed.astype(jnp.bfloat16).astype(jnp.float32)
    mixed_low = mixed - mixed_high
    last = jnp.where(lane < 32, mixed_high[:, LANES:], 0.0)
    last = last + pltpu.roll(jnp.where(lane < 32, mixed_low[:, LANES:], 0.0), 32, 1)
    left_side = jnp.concatenate(
        [summed, mixed_high[:, 0:LANES], mixed_low[:, 0:LANES], last], 1
    ).astype(jnp.bfloat16)

    flip_ref[...] = jnp.zeros(flip_ref.shape, jnp.float32)
    lane1 = iota((1, LANES), 1)
    own_col = own_ref[CH + 1 : CH + 2, :]
    thrice = own_col + pltpu.roll(jnp.broadcast_to(own_col, (8, LANES)), 32, 1)[0:1, :]
    thrice = thrice + pltpu.roll(jnp.broadcast_to(own_col, (8, LANES)), 64, 1)[0:1, :]
    flip_ref[0:1, :] = jnp.where(lane1 < 96, thrice, float(NOWHERE))
    flip_ref[1:2, :] = four[CH + 1 : CH + 2, :]
    flip_ref[2:3, :] = four[CH + 2 : CH + 3, :]
    down_col = jnp.broadcast_to(down_ref[CH + 1 : CH + 2, :], (8, LANES))
    down_on = jnp.broadcast_to(down_ref[CH + 2 : CH + 3, :], (8, LANES))
    flip_ref[3:4, :] = (down_col + pltpu.roll(down_col, 32, 1))[0:1, :]
    flip_ref[4:5, :] = (down_on + pltpu.roll(down_on, 32, 1))[0:1, :]
    flipped = jnp.transpose(flip_ref[...])
    col3 = jnp.broadcast_to(flipped[:, 0:1], (LANES, LANES)).astype(jnp.int32)
    col = jnp.broadcast_to(flipped[:, 1:2], (LANES, LANES)).astype(jnp.int32)
    on = jnp.broadcast_to(flipped[:, 2:3], (LANES, LANES))
    col_down = jnp.broadcast_to(flipped[:, 3:4], (LANES, LANES)).astype(jnp.int32)
    on_down = jnp.broadcast_to(flipped[:, 4:5], (LANES, LANES))
    across = iota((LANES, LANES), 1)
    spot = iota((32, LANES), 1)
    none = jnp.zeros((32, LANES), jnp.float32)

    def right_side(r):
        point = across + r * LANES
        pick = jnp.where(col3 == point, 1.0, 0.0)
        mine, lefts, rights, ups = (col[32 * i : 32 * (i + 1), :] for i in range(4))
        here = spot + r * LANES
        stencil = jnp.where(mine == here, -4.0, 0.0)
        stencil = stencil + jnp.where((mine == here - 1) & (spot != 0), 1.0, 0.0)
        stencil = stencil + jnp.where((mine == here + 1) & (spot != LANES - 1), 1.0, 0.0)
        stencil = stencil + jnp.where((mine == here - LANES) | (mine == here + LANES), 1.0, 0.0)
        to_left = jnp.where((spot == 0) & (lefts == r * LANES + LANES - 1), 1.0, 0.0)
        to_right = jnp.where((spot == LANES - 1) & (rights == r * LANES), 1.0, 0.0)
        to_up = jnp.where(ups == spot + (ROWS - 1) * LANES, 1.0, 0.0) if r == 0 else none
        reach = jnp.concatenate([stencil, to_left, to_right, to_up], 0) * on
        if r == ROWS - 1:
            to_down = jnp.where(col_down == across, 1.0, 0.0) * on_down
        else:
            to_down = jnp.zeros((LANES, LANES), jnp.float32)
        return jnp.concatenate([pick, reach, reach, to_down], 0).astype(jnp.bfloat16)

    for r in range(0, ROWS, 2):
        pair = jnp.concatenate([right_side(r), right_side(r + 1)], 1)
        added = jnp.dot(left_side, pair, preferred_element_type=jnp.float32)
        for i in range(2):
            rows = pl.ds(r + i, depth, stride=ROWS)
            out_ref[rows, :] = inc_ref[rows, :] + added[:, i * LANES : (i + 1) * LANES]


def moved(x, axis, step, periodic):
    count = lax.axis_size(axis)
    pairs = [(i, (i + step) % count) for i in range(count) if periodic or 0 <= i + step < count]
    return lax.ppermute(x, axis, pairs)


def on_device(increment, mixing, mixing_mask, jacobian, fp_col, fp_class, obs, obs_weight):
    f32 = jnp.float32
    peers = lax.axis_size("lat")
    depth = 2 * increment.shape[1]
    slots = fp_col.shape[2]
    kinds = jacobian.shape[0] * CH
    inc = increment.reshape(depth * ROWS, LANES)
    mix = mixing.reshape(depth, 1)
    jac = jnp.transpose(jacobian, (1, 0, 2)).reshape(kinds, depth)
    turned_jac = jnp.transpose(jac)
    struct = jax.ShapeDtypeStruct

    records = call(
        records_body, struct((peers, 1, SLOT * STRIDE), f32),
        (pltpu.VMEM((LANES, slots), f32), pltpu.VMEM((slots, LANES), f32), pltpu.VMEM((peers, SLOT * STRIDE), f32)),
    )(obs.reshape(CH, 1, slots), obs_weight.reshape(CH, 1, slots), fp_class)
    records = lax.all_to_all(records, "lat", split_axis=0, concat_axis=0, tiled=True)

    edge = struct((depth, LANES), f32)
    first, last, to_right, to_left = call(edges_body, (edge, edge, edge, edge))(inc)
    up = moved(last, "lat", 1, False)
    down = moved(first, "lat", -1, False)
    from_left = moved(to_right, "lon", 1, True)
    from_right = moved(to_left, "lon", -1, True)

    seen, meta = call(
        state_body, (struct((kinds, LANES), f32), struct((8, LANES), f32)),
    )(inc, up, down, from_left, from_right, fp_col.reshape(1, slots), mixing_mask, mix, jac)
    own = call(
        departures_body, struct((24, LANES), f32),
        (pltpu.VMEM((8, SLOT * STRIDE), f32), pltpu.VMEM((LANES, LANES), f32)),
    )(records, seen, meta)

    above = moved(own, "lat", 1, False)
    below = moved(own, "lat", -1, False)
    lefts = moved(own, "lon", 1, True)
    rights = moved(own, "lon", -1, True)
    out = call(
        gradient_body, struct((depth * ROWS, LANES), f32),
        (pltpu.VMEM((kinds, 2 * LANES), f32), pltpu.VMEM((LANES, LANES), f32)),
    )(own, lefts, rights, above, below, turned_jac, mix, inc)
    return out.reshape(increment.shape)


def solution(mesh):
    return jax.shard_map(
        on_device,
        mesh=mesh,
        in_specs=(
            P(None, None, "lat", "lon"),
            P(),
            P("lat", "lon"),
            P(),
            P("lon", "lat", None),
            P("lon", "lat", None),
            P("lon", "lat", None, None),
            P("lon", "lat", None, None),
        ),
        out_specs=P(None, None, "lat", "lon"),
        check_vma=False,
    )
```

```python
import jax
import jax.numpy as jnp
from jax import lax
from jax.experimental import pallas as pl
from jax.experimental.pallas import tpu as pltpu
from jax.sharding import PartitionSpec as P

OWN_EVERY = 8
SLOT = 8
ROWS = 8
LANES = 128
STRIDE = 48
CH = 20
NOWHERE = -1000000


def iota(shape, dim):
    return lax.broadcasted_iota(jnp.int32, shape, dim)


def call(body, out_shape, scratch=(), flops=1000000, inputs=1, limit=16 * 1024 * 1024):
    vmem = pl.BlockSpec(memory_space=pltpu.VMEM)
    return pl.pallas_call(
        body,
        out_shape=out_shape,
        in_specs=[vmem] * inputs,
        out_specs=jax.tree.map(lambda _: vmem, out_shape),
        scratch_shapes=list(scratch),
        compiler_params=pltpu.CompilerParams(vmem_limit_bytes=limit),
        cost_estimate=pl.CostEstimate(flops=flops, bytes_accessed=1000000, transcendentals=0),
    )


def record_spots():
    return [((k * STRIDE) // LANES, (k * STRIDE) % LANES) for k in range(SLOT)]


def records_body(obs_ref, weight_ref, class_ref, out_ref, wide_ref, tall_ref, flat_ref):
    peers = out_ref.shape[0]
    wide_ref[...] = jnp.zeros(wide_ref.shape, jnp.float32)
    for ch in range(CH):
        wide_ref[ch : ch + 1, :] = obs_ref[ch]
        wide_ref[24 + ch : 25 + ch, :] = weight_ref[ch]
    wide_ref[CH : CH + 1, :] = class_ref[0].astype(jnp.float32)
    tall_ref[...] = jnp.transpose(wide_ref[...])
    lane = iota((peers, LANES), 1)
    tiles = [jnp.zeros((peers, LANES), jnp.float32) for _ in range(SLOT * STRIDE // LANES)]
    for k, (tile, off) in enumerate(record_spots()):
        part = tall_ref[pl.ds(k, peers, stride=SLOT), :]
        part = pltpu.roll(part, off, 1) if off else part
        if off + STRIDE <= LANES:
            tiles[tile] = tiles[tile] + part
        else:
            tiles[tile] = tiles[tile] + jnp.where(lane >= off, part, 0.0)
            tiles[tile + 1] = tiles[tile + 1] + jnp.where(lane < off, part, 0.0)
    for i, value in enumerate(tiles):
        flat_ref[:, i * LANES : (i + 1) * LANES] = value
    for s in range(peers):
        out_ref[s] = flat_ref[s : s + 1, :]


def is_even(axis):
    return lax.axis_index(axis) % 2 == 0


def edges_body(inc_ref, lon_ref, lat_ref, lat2_ref, lon2_ref):
    depth = lon_ref.shape[0]
    lane = iota((depth, LANES), 1)
    right = jnp.zeros((depth, LANES), jnp.float32)
    left = jnp.zeros((depth, LANES), jnp.float32)
    for r in range(ROWS):
        row = inc_ref[pl.ds(r, depth, stride=ROWS), :]
        if r == 0:
            first = row
        if r == ROWS - 1:
            last = row
        right = jnp.where(lane == r, pltpu.roll(row, r + 1, 1), right)
        left = jnp.where(lane == ROWS + r, pltpu.roll(row, ROWS + r, 1), left)
    even = is_even("lat")
    lat_ref[...] = jnp.where(even, last, first)
    lat2_ref[...] = jnp.where(even, first, last)
    even = is_even("lon")
    lon_ref[...] = jnp.where(even, right, left)
    lon2_ref[...] = jnp.where(even, left, right)


def state_body(inc_ref, lon_ref, lat_ref, lat2_ref, lon2_ref, col_ref, mask_ref, mix_ref,
               jac_ref, seen_ref, meta_ref):
    depth = lat_ref.shape[0]
    lane8 = iota((8, LANES), 1)
    cols = jnp.full((8, LANES), NOWHERE, jnp.int32)
    owners = col_ref.shape[1] // (SLOT * OWN_EVERY)
    for g in range(owners):
        start = g * SLOT * OWN_EVERY
        tile = jnp.broadcast_to(col_ref[:, start // LANES * LANES : start // LANES * LANES + LANES], (8, LANES))
        shift = (g * SLOT - start % LANES) % LANES
        tile = pltpu.roll(tile, shift, 1) if shift else tile
        cols = jnp.where((lane8 >= g * SLOT) & (lane8 < (g + 1) * SLOT), tile, cols)
    cols = jnp.where(cols >= 0, cols, NOWHERE)
    both = jnp.where(lane8 < 32, cols, jnp.where(lane8 < 64, pltpu.roll(cols, 32, 1), NOWHERE))
    want = jnp.broadcast_to(both[0:1, :], (LANES, LANES))
    sub = iota((LANES, LANES), 0)
    plain = iota((LANES, LANES), 1) < 32

    def split_dot(x, chosen):
        high = x.astype(jnp.bfloat16)
        low = (x - high.astype(jnp.float32)).astype(jnp.bfloat16)
        return jnp.dot(
            jnp.concatenate([high, low], 1), jnp.concatenate([chosen, chosen], 0),
            preferred_element_type=jnp.float32,
        )

    total = jnp.zeros((depth, LANES), jnp.float32)
    masked = jnp.zeros((8, LANES), jnp.float32)
    for r in range(ROWS):
        point = sub + r * LANES
        here = jnp.where(want == point, 1.0, 0.0)
        beside = jnp.where((want == point - 1) & (sub != 0), 1.0, 0.0)
        beside = beside + jnp.where((want == point + 1) & (sub != LANES - 1), 1.0, 0.0)
        beside = beside + jnp.where((want == point - LANES) | (want == point + LANES), 1.0, 0.0)
        chosen = jnp.where(plain, here, beside - 4.0 * here).astype(jnp.bfloat16)
        total = total + split_dot(inc_ref[pl.ds(r, depth, stride=ROWS), :], chosen)
        mask_row = jnp.broadcast_to(mask_ref[r : r + 1, :].astype(jnp.bfloat16), (8, LANES))
        masked = masked + jnp.dot(mask_row, chosen, preferred_element_type=jnp.float32)
    near = ~plain
    meets = jnp.where(is_even("lat"), (ROWS - 1) * LANES, 0)
    chosen = jnp.where(near & (want == sub + meets), 1.0, 0.0).astype(jnp.bfloat16)
    total = total + split_dot(lat_ref[...], chosen)
    chosen = jnp.where(near & (want == sub + ((ROWS - 1) * LANES - meets)), 1.0, 0.0).astype(jnp.bfloat16)
    total = total + split_dot(lat2_ref[...], chosen)
    on_left = (sub < ROWS) & (want == sub * LANES)
    on_right = (sub >= ROWS) & (sub < 2 * ROWS) & (want == (sub - ROWS) * LANES + LANES - 1)
    chosen = jnp.where(near & (on_left | on_right), 1.0, 0.0).astype(jnp.bfloat16)
    total = total + split_dot(lon_ref[...] + lon2_ref[...], chosen)

    state = total + mix_ref[...] * masked[0:1, :] * pltpu.roll(total, LANES - 32, 1)
    state = jnp.where(iota((depth, LANES), 1) < 32, state, 0.0).astype(jnp.bfloat16)
    seen_ref[...] = jnp.dot(jac_ref[...], state, preferred_element_type=jnp.float32)
    meta_ref[0:1, :] = cols[0:1, :].astype(jnp.float32)
    meta_ref[1:2, :] = masked[0:1, :]
    meta_ref[2:8, :] = jnp.zeros((6, LANES), jnp.float32)


def departures_body(records_ref, seen_ref, meta_ref, out_ref, row_ref, spot_ref):
    owners = records_ref.shape[0] // OWN_EVERY
    classes = seen_ref.shape[0] // CH
    row_ref[...] = jnp.zeros(row_ref.shape, jnp.float32)
    spot_ref[...] = jnp.zeros(spot_ref.shape, jnp.float32)
    for g in range(owners):
        row_ref[g : g + 1, :] = records_ref[g * OWN_EVERY]
    lane8 = iota((8, LANES), 1)
    tiles = [row_ref[:, i * LANES : (i + 1) * LANES] for i in range(SLOT * STRIDE // LANES)]
    for k, (tile, off) in enumerate(record_spots()):
        part = pltpu.roll(tiles[tile], LANES - off, 1) if off else tiles[tile]
        if off + STRIDE > LANES:
            part = jnp.where(lane8 < LANES - off, part, pltpu.roll(tiles[tile + 1], LANES - off, 1))
        for g in range(owners):
            spot_ref[g * SLOT + k : g * SLOT + k + 1, :] = part[g : g + 1, :]
    turned = jnp.transpose(spot_ref[...])
    lane1 = iota((1, LANES), 1)
    kind = jnp.where(lane1 < owners * SLOT, turned[CH : CH + 1, :], -1.0)
    chosen = jnp.broadcast_to(kind, (classes, LANES)).astype(jnp.int32) == iota((classes, LANES), 0)
    out_ref[...] = jnp.zeros(out_ref.shape, jnp.float32)
    for ch in range(CH):
        rows = seen_ref[ch * classes : (ch + 1) * classes, :]
        out_ref[ch : ch + 1, :] = jnp.sum(jnp.where(chosen, rows, 0.0), axis=0, keepdims=True)
    evolved = out_ref[0:CH, :]
    weighted = turned[24 : 24 + CH, :] * (evolved - turned[0:CH, :])
    weighted = jnp.where(jnp.broadcast_to(kind, (CH, LANES)) >= 0, weighted, 0.0)
    out_ref[0:CH, :] = weighted.astype(jnp.bfloat16).astype(jnp.float32)
    live = lane1 < owners * SLOT
    out_ref[CH : CH + 1, :] = jnp.where(live, kind, 0.0)
    out_ref[CH + 1 : CH + 2, :] = jnp.where(live, meta_ref[0:1, :], 0.0)
    out_ref[CH + 2 : CH + 3, :] = jnp.where(live, meta_ref[1:2, :], 0.0)
    col = meta_ref[0:1, :].astype(jnp.int32)
    across = col & (LANES - 1)
    ahead = [
        jnp.where(across == LANES - 1, col - (LANES - 1), NOWHERE),
        jnp.where(col >= (ROWS - 1) * LANES, col - (ROWS - 1) * LANES, NOWHERE),
    ]
    behind = [
        jnp.where(across == 0, col + (LANES - 1), NOWHERE),
        jnp.where((col >= 0) & (col < LANES), col + (ROWS - 1) * LANES, NOWHERE),
    ]
    for i, axis in enumerate(("lon", "lat")):
        even = is_even(axis)
        for j, swap in enumerate((even, jnp.logical_not(even))):
            spot = jnp.where(swap, ahead[i], behind[i]).astype(jnp.float32)
            row = CH + 3 + 2 * i + j
            out_ref[row : row + 1, :] = jnp.where(live, spot, 0.0)


def gradient_body(own_ref, lon2_ref, lat2_ref, lat_ref, lon_ref, turned_jac_ref, mix_ref, inc_ref,
                  out_ref, spread_ref, flip_ref):
    depth = turned_jac_ref.shape[0]
    classes = turned_jac_ref.shape[1] // CH
    lon = pltpu.roll(lon_ref[...], 32, 1)
    lon2 = pltpu.roll(lon2_ref[...], 64, 1)
    lat = pltpu.roll(lat_ref[...], 96, 1)
    four = own_ref[...] + lon + lon2 + lat
    both = jnp.concatenate([four, lat2_ref[...]], 1)
    kinds = jnp.broadcast_to(both[CH : CH + 1, :], (classes, 2 * LANES)).astype(jnp.int32)
    chosen = kinds == iota((classes, 2 * LANES), 0)
    for ch in range(CH):
        spread_ref[ch * classes : (ch + 1) * classes, :] = jnp.where(chosen, both[ch : ch + 1, :], 0.0)
    adjoint = jnp.dot(turned_jac_ref[...], spread_ref[...].astype(jnp.bfloat16), preferred_element_type=jnp.float32)

    lane = iota((depth, LANES), 1)
    own = jnp.where(lane < 32, adjoint[:, 0:LANES], 0.0)
    own_high = own.astype(jnp.bfloat16).astype(jnp.float32)
    rest = own - own_high
    own_mid = rest.astype(jnp.bfloat16).astype(jnp.float32)
    own_low = rest - own_mid
    summed = own_high + pltpu.roll(own_mid, 32, 1) + pltpu.roll(own_low, 64, 1)
    mixed = mix_ref[...] * adjoint
    mixed_high = mixed.astype(jnp.bfloat16).astype(jnp.float32)
    mixed_low = mixed - mixed_high
    last = jnp.where(lane < 32, mixed_high[:, LANES:], 0.0)
    last = last + pltpu.roll(jnp.where(lane < 32, mixed_low[:, LANES:], 0.0), 32, 1)
    left_side = jnp.concatenate(
        [summed, mixed_high[:, 0:LANES], mixed_low[:, 0:LANES], last], 1
    ).astype(jnp.bfloat16)

    flip_ref[...] = jnp.zeros(flip_ref.shape, jnp.float32)
    lane8 = iota((8, LANES), 1)
    own_col = jnp.broadcast_to(own_ref[CH + 1 : CH + 2, :], (8, LANES))
    thrice = own_col + pltpu.roll(own_col, 32, 1) + pltpu.roll(own_col, 64, 1)
    flip_ref[0:8, :] = jnp.where(lane8 < 96, thrice, float(NOWHERE))
    spots = own_ref[CH + 1 : CH + 2, :] + lon[CH + 3 : CH + 4, :] + lon2[CH + 4 : CH + 5, :] + lat[CH + 5 : CH + 6, :]
    flip_ref[1:2, :] = spots
    flip_ref[2:3, :] = four[CH + 2 : CH + 3, :]
    lat2_spot = jnp.broadcast_to(lat2_ref[CH + 6 : CH + 7, :], (8, LANES))
    lat2_on = jnp.broadcast_to(lat2_ref[CH + 2 : CH + 3, :], (8, LANES))
    flip_ref[3:4, :] = (lat2_spot + pltpu.roll(lat2_spot, 32, 1))[0:1, :]
    flip_ref[4:5, :] = (lat2_on + pltpu.roll(lat2_on, 32, 1))[0:1, :]
    flipped = jnp.transpose(flip_ref[...])
    col3 = jnp.broadcast_to(flipped[:, 0:1], (LANES, LANES)).astype(jnp.int32)
    col = jnp.broadcast_to(flipped[:, 1:2], (LANES, LANES)).astype(jnp.int32)
    on = jnp.broadcast_to(flipped[:, 2:3], (LANES, LANES))
    col_last = jnp.broadcast_to(flipped[:, 3:4], (LANES, LANES)).astype(jnp.int32)
    on_last = jnp.broadcast_to(flipped[:, 4:5], (LANES, LANES))
    across = iota((LANES, LANES), 1)
    spot = iota((32, LANES), 1)
    mine = col[0:32, :]

    def right_side(r):
        point = across + r * LANES
        pick = jnp.where(col3 == point, 1.0, 0.0)
        here = spot + r * LANES
        stencil = jnp.where(mine == here, -4.0, 0.0)
        stencil = stencil + jnp.where((mine == here - 1) & (spot != 0), 1.0, 0.0)
        stencil = stencil + jnp.where((mine == here + 1) & (spot != LANES - 1), 1.0, 0.0)
        stencil = stencil + jnp.where((mine == here - LANES) | (mine == here + LANES), 1.0, 0.0)
        given = jnp.where(col[32:LANES, :] == point[32:LANES, :], 1.0, 0.0)
        reach = jnp.concatenate([stencil, given], 0) * on
        reach_last = jnp.where(col_last == point, on_last, 0.0)
        return jnp.concatenate([pick, reach, reach, reach_last], 0).astype(jnp.bfloat16)

    for r in range(0, ROWS, 2):
        pair = jnp.concatenate([right_side(r), right_side(r + 1)], 1)
        added = jnp.dot(left_side, pair, preferred_element_type=jnp.float32)
        for i in range(2):
            rows = pl.ds(r + i, depth, stride=ROWS)
            out_ref[rows, :] = inc_ref[rows, :] + added[:, i * LANES : (i + 1) * LANES]


def swapped(x, axis, start, periodic):
    count = lax.axis_size(axis)
    pairs = []
    for i in range(start, count, 2):
        if periodic or i + 1 < count:
            pairs += [(i, (i + 1) % count), ((i + 1) % count, i)]
    return lax.ppermute(x, axis, pairs)


def on_device(increment, mixing, mixing_mask, jacobian, fp_col, fp_class, obs, obs_weight):
    f32 = jnp.float32
    peers = lax.axis_size("lat")
    depth = 2 * increment.shape[1]
    slots = fp_col.shape[2]
    kinds = jacobian.shape[0] * CH
    inc = increment.reshape(depth * ROWS, LANES)
    mix = mixing.reshape(depth, 1)
    jac = jnp.transpose(jacobian, (1, 0, 2)).reshape(kinds, depth)
    turned_jac = jnp.transpose(jac)
    struct = jax.ShapeDtypeStruct

    records = call(
        records_body, struct((peers, 1, SLOT * STRIDE), f32),
        (pltpu.VMEM((LANES, slots), f32), pltpu.VMEM((slots, LANES), f32), pltpu.VMEM((peers, SLOT * STRIDE), f32)),
        inputs=3, limit=None,
    )(obs.reshape(CH, 1, slots), obs_weight.reshape(CH, 1, slots), fp_class)
    records = lax.all_to_all(records, "lat", split_axis=0, concat_axis=0, tiled=True)

    edge = struct((depth, LANES), f32)
    edges = call(edges_body, (edge, edge, edge, edge))(inc)
    swaps = (("lon", 0, True), ("lat", 0, False), ("lat", 1, False), ("lon", 1, True))
    edges = [swapped(x, *swap) for x, swap in zip(edges, swaps)]

    seen, meta = call(
        state_body, (struct((kinds, LANES), f32), struct((8, LANES), f32)), inputs=9,
    )(inc, *edges, fp_col.reshape(1, slots), mixing_mask, mix, jac)
    own = call(
        departures_body, struct((32, LANES), f32),
        (pltpu.VMEM((8, SLOT * STRIDE), f32), pltpu.VMEM((LANES, LANES), f32)), inputs=3,
    )(records, seen, meta)

    out = call(
        gradient_body, struct((depth * ROWS, LANES), f32),
        (pltpu.VMEM((kinds, 2 * LANES), f32), pltpu.VMEM((LANES, LANES), f32)), inputs=8,
    )(own, *(swapped(own, *swap) for swap in swaps[::-1]), turned_jac, mix, inc)
    return out.reshape(increment.shape)


def solution(mesh):
    return jax.shard_map(
        on_device,
        mesh=mesh,
        in_specs=(
            P(None, None, "lat", "lon"),
            P(),
            P("lat", "lon"),
            P(),
            P("lon", "lat", None),
            P("lon", "lat", None),
            P("lon", "lat", None, None),
            P("lon", "lat", None, None),
        ),
        out_specs=P(None, None, "lat", "lon"),
        check_vma=False,
    )
```

```python
import jax
import jax.numpy as jnp
from jax import lax
from jax.experimental import pallas as pl
from jax.experimental.pallas import tpu as pltpu
from jax.sharding import PartitionSpec as P

OWN_EVERY = 8
SLOT = 8
ROWS = 8
LANES = 128
STRIDE = 48
CH = 20
NOWHERE = -1000000
CHUNK = 96


def iota(shape, dim):
    return lax.broadcasted_iota(jnp.int32, shape, dim)


def call(body, out_shape, scratch=(), flops=1000000, inputs=1, limit=16 * 1024 * 1024, space=pltpu.VMEM):
    vmem = pl.BlockSpec(memory_space=pltpu.VMEM)
    return pl.pallas_call(
        body,
        out_shape=out_shape,
        in_specs=[vmem] * inputs,
        out_specs=jax.tree.map(lambda _: pl.BlockSpec(memory_space=space), out_shape),
        scratch_shapes=list(scratch),
        compiler_params=pltpu.CompilerParams(vmem_limit_bytes=limit),
        cost_estimate=pl.CostEstimate(flops=flops, bytes_accessed=1000000, transcendentals=0),
    )


def record_spots():
    return [((k * STRIDE) // LANES, (k * STRIDE) % LANES) for k in range(SLOT)]


def records_body(obs_ref, weight_ref, class_ref, out_ref, wide_ref, tall_ref, flat_ref):
    peers = out_ref.shape[0]
    wide_ref[...] = jnp.zeros(wide_ref.shape, jnp.float32)
    for ch in range(CH):
        wide_ref[ch : ch + 1, :] = obs_ref[ch]
        wide_ref[24 + ch : 25 + ch, :] = weight_ref[ch]
    wide_ref[CH : CH + 1, :] = class_ref[0].astype(jnp.float32)
    tall_ref[...] = jnp.transpose(wide_ref[...])
    lane = iota((peers, LANES), 1)
    tiles = [jnp.zeros((peers, LANES), jnp.float32) for _ in range(SLOT * STRIDE // LANES)]
    for k, (tile, off) in enumerate(record_spots()):
        part = tall_ref[pl.ds(k, peers, stride=SLOT), :]
        part = pltpu.roll(part, off, 1) if off else part
        if off + STRIDE <= LANES:
            tiles[tile] = tiles[tile] + part
        else:
            tiles[tile] = tiles[tile] + jnp.where(lane >= off, part, 0.0)
            tiles[tile + 1] = tiles[tile + 1] + jnp.where(lane < off, part, 0.0)
    for i, value in enumerate(tiles):
        flat_ref[:, i * LANES : (i + 1) * LANES] = value
    for s in range(peers):
        out_ref[s] = flat_ref[s : s + 1, :]


def is_even(axis):
    return lax.axis_index(axis) % 2 == 0


def edges_body(inc_ref, lon2_ref, lat_ref, lat2_ref, lon_ref):
    depth = lon_ref.shape[0]
    lane = iota((depth, LANES), 1)
    right = jnp.zeros((depth, LANES), jnp.float32)
    left = jnp.zeros((depth, LANES), jnp.float32)
    for r in range(ROWS):
        row = inc_ref[pl.ds(r, depth, stride=ROWS), :]
        if r == 0:
            first = row
        if r == ROWS - 1:
            last = row
        right = jnp.where(lane == r, pltpu.roll(row, r + 1, 1), right)
        left = jnp.where(lane == ROWS + r, pltpu.roll(row, ROWS + r, 1), left)
    even = is_even("lat")
    lat_ref[...] = jnp.where(even, last, first)
    lat2_ref[...] = jnp.where(even, first, last)
    even = is_even("lon")
    lon_ref[...] = jnp.where(even, right, left)
    lon2_ref[...] = jnp.where(even, left, right)


def state_body(inc_ref, lon2_ref, lat_ref, lat2_ref, lon_ref, col_ref, mask_ref, mix_ref,
               jac_ref, seen_ref, meta_ref):
    depth = lat_ref.shape[0]
    lane8 = iota((8, LANES), 1)
    cols = jnp.full((8, LANES), NOWHERE, jnp.int32)
    owners = col_ref.shape[1] // (SLOT * OWN_EVERY)
    for g in range(owners):
        start = g * SLOT * OWN_EVERY
        tile = jnp.broadcast_to(col_ref[:, start // LANES * LANES : start // LANES * LANES + LANES], (8, LANES))
        shift = (g * SLOT - start % LANES) % LANES
        tile = pltpu.roll(tile, shift, 1) if shift else tile
        cols = jnp.where((lane8 >= g * SLOT) & (lane8 < (g + 1) * SLOT), tile, cols)
    cols = jnp.where(cols >= 0, cols, NOWHERE)
    both = jnp.where(lane8 < 32, cols, jnp.where(lane8 < 64, pltpu.roll(cols, 32, 1), NOWHERE))
    want = jnp.broadcast_to(both[0:1, :], (LANES, LANES))
    sub = iota((LANES, LANES), 0)
    plain = iota((LANES, LANES), 1) < 32

    def split_dot(x, chosen):
        high = x.astype(jnp.bfloat16)
        low = (x - high.astype(jnp.float32)).astype(jnp.bfloat16)
        return jnp.dot(
            jnp.concatenate([high, low], 1), jnp.concatenate([chosen, chosen], 0),
            preferred_element_type=jnp.float32,
        )

    total = jnp.zeros((depth, LANES), jnp.float32)
    masked = jnp.zeros((8, LANES), jnp.float32)
    for r in range(ROWS):
        point = sub + r * LANES
        here = jnp.where(want == point, 1.0, 0.0)
        beside = jnp.where((want == point - 1) & (sub != 0), 1.0, 0.0)
        beside = beside + jnp.where((want == point + 1) & (sub != LANES - 1), 1.0, 0.0)
        beside = beside + jnp.where((want == point - LANES) | (want == point + LANES), 1.0, 0.0)
        chosen = jnp.where(plain, here, beside - 4.0 * here).astype(jnp.bfloat16)
        total = total + split_dot(inc_ref[pl.ds(r, depth, stride=ROWS), :], chosen)
        mask_row = jnp.broadcast_to(mask_ref[r : r + 1, :].astype(jnp.bfloat16), (8, LANES))
        masked = masked + jnp.dot(mask_row, chosen, preferred_element_type=jnp.float32)
    near = ~plain
    meets = jnp.where(is_even("lat"), (ROWS - 1) * LANES, 0)
    chosen = jnp.where(near & (want == sub + meets), 1.0, 0.0).astype(jnp.bfloat16)
    total = total + split_dot(lat_ref[...], chosen)
    chosen = jnp.where(near & (want == sub + ((ROWS - 1) * LANES - meets)), 1.0, 0.0).astype(jnp.bfloat16)
    total = total + split_dot(lat2_ref[...], chosen)
    on_left = (sub < ROWS) & (want == sub * LANES)
    on_right = (sub >= ROWS) & (sub < 2 * ROWS) & (want == (sub - ROWS) * LANES + LANES - 1)
    chosen = jnp.where(near & (on_left | on_right), 1.0, 0.0).astype(jnp.bfloat16)
    total = total + split_dot(lon_ref[...] + lon2_ref[...], chosen)

    state = total + mix_ref[...] * masked[0:1, :] * pltpu.roll(total, LANES - 32, 1)
    state = jnp.where(iota((depth, LANES), 1) < 32, state, 0.0).astype(jnp.bfloat16)
    seen_ref[...] = jnp.dot(jac_ref[...], state, preferred_element_type=jnp.float32)
    meta_ref[0:1, :] = cols[0:1, :].astype(jnp.float32)
    meta_ref[1:2, :] = masked[0:1, :]
    meta_ref[2:8, :] = jnp.zeros((6, LANES), jnp.float32)


def departures_body(records_ref, seen_ref, meta_ref, out_ref, row_ref, spot_ref):
    owners = records_ref.shape[0] // OWN_EVERY
    classes = seen_ref.shape[0] // CH
    row_ref[...] = jnp.zeros(row_ref.shape, jnp.float32)
    spot_ref[...] = jnp.zeros(spot_ref.shape, jnp.float32)
    for g in range(owners):
        row_ref[g : g + 1, :] = records_ref[g * OWN_EVERY]
    lane8 = iota((8, LANES), 1)
    tiles = [row_ref[:, i * LANES : (i + 1) * LANES] for i in range(SLOT * STRIDE // LANES)]
    for k, (tile, off) in enumerate(record_spots()):
        part = pltpu.roll(tiles[tile], LANES - off, 1) if off else tiles[tile]
        if off + STRIDE > LANES:
            part = jnp.where(lane8 < LANES - off, part, pltpu.roll(tiles[tile + 1], LANES - off, 1))
        for g in range(owners):
            spot_ref[g * SLOT + k : g * SLOT + k + 1, :] = part[g : g + 1, :]
    turned = jnp.transpose(spot_ref[...])
    lane1 = iota((1, LANES), 1)
    kind = jnp.where(lane1 < owners * SLOT, turned[CH : CH + 1, :], -1.0)
    chosen = jnp.broadcast_to(kind, (classes, LANES)).astype(jnp.int32) == iota((classes, LANES), 0)
    out_ref[...] = jnp.zeros(out_ref.shape, jnp.float32)
    for ch in range(CH):
        rows = seen_ref[ch * classes : (ch + 1) * classes, :]
        out_ref[ch : ch + 1, :] = jnp.sum(jnp.where(chosen, rows, 0.0), axis=0, keepdims=True)
    evolved = out_ref[0:CH, :]
    weighted = turned[24 : 24 + CH, :] * (evolved - turned[0:CH, :])
    weighted = jnp.where(jnp.broadcast_to(kind, (CH, LANES)) >= 0, weighted, 0.0)
    out_ref[0:CH, :] = weighted.astype(jnp.bfloat16).astype(jnp.float32)
    live = lane1 < owners * SLOT
    out_ref[CH : CH + 1, :] = jnp.where(live, kind, 0.0)
    out_ref[CH + 1 : CH + 2, :] = jnp.where(live, meta_ref[0:1, :], 0.0)
    out_ref[CH + 2 : CH + 3, :] = jnp.where(live, meta_ref[1:2, :], 0.0)
    col = meta_ref[0:1, :].astype(jnp.int32)
    across = col & (LANES - 1)
    ahead = [
        jnp.where(across == LANES - 1, col - (LANES - 1), NOWHERE),
        jnp.where(col >= (ROWS - 1) * LANES, col - (ROWS - 1) * LANES, NOWHERE),
    ]
    behind = [
        jnp.where(across == 0, col + (LANES - 1), NOWHERE),
        jnp.where((col >= 0) & (col < LANES), col + (ROWS - 1) * LANES, NOWHERE),
    ]
    for i, axis in enumerate(("lon", "lat")):
        even = is_even(axis)
        for j, swap in enumerate((even, jnp.logical_not(even))):
            spot = jnp.where(swap, ahead[i], behind[i]).astype(jnp.float32)
            row = CH + 3 + 2 * i + j
            out_ref[row : row + 1, :] = jnp.where(live, spot, 0.0)


def gradient_body(own_ref, lon_ref, lat2_ref, lat_ref, lon2_ref, turned_jac_ref, mix_ref, inc_ref,
                  out_hbm, spread_ref, flip_ref, out_ref, sems):
    depth = turned_jac_ref.shape[0]
    classes = turned_jac_ref.shape[1] // CH
    met = [ref[...] if i == 0 else pltpu.roll(ref[...], 32 * i, 1)
           for i, ref in enumerate((lon_ref, lon2_ref, lat_ref, lat2_ref))]
    others = met[0] + met[1] + met[2] + met[3]
    both = jnp.concatenate([own_ref[...], others], 1)
    kinds = jnp.broadcast_to(both[CH : CH + 1, :], (classes, 2 * LANES)).astype(jnp.int32)
    chosen = kinds == iota((classes, 2 * LANES), 0)
    for ch in range(CH):
        spread_ref[ch * classes : (ch + 1) * classes, :] = jnp.where(chosen, both[ch : ch + 1, :], 0.0)
    adjoint = jnp.dot(turned_jac_ref[...], spread_ref[...].astype(jnp.bfloat16), preferred_element_type=jnp.float32)

    own = jnp.where(iota((depth, LANES), 1) < 32, adjoint[:, 0:LANES], 0.0)
    own_high = own.astype(jnp.bfloat16).astype(jnp.float32)
    mixed = mix_ref[...] * own
    mixed_high = mixed.astype(jnp.bfloat16).astype(jnp.float32)
    parts = own_high + pltpu.roll(own - own_high, 32, 1)
    parts = parts + pltpu.roll(mixed_high, 64, 1) + pltpu.roll(mixed - mixed_high, 96, 1)
    left_side = jnp.concatenate([parts, mix_ref[...] * adjoint[:, LANES:]], 1).astype(jnp.bfloat16)

    flip_ref[...] = jnp.zeros(flip_ref.shape, jnp.float32)
    flip_ref[0:1, :] = own_ref[CH + 1 : CH + 2, :]
    flip_ref[1:2, :] = own_ref[CH + 2 : CH + 3, :]
    flip_ref[2:3, :] = sum(met[i][CH + 3 + n : CH + 4 + n, :] for i, n in enumerate((0, 1, 2, 3)))
    flip_ref[3:4, :] = others[CH + 2 : CH + 3, :]
    flipped = jnp.transpose(flip_ref[...])
    mine = jnp.broadcast_to(flipped[0:32, 0:1], (32, LANES)).astype(jnp.int32)
    on = jnp.broadcast_to(flipped[0:32, 1:2], (32, LANES))
    theirs = jnp.broadcast_to(flipped[:, 2:3], (LANES, LANES)).astype(jnp.int32)
    on_theirs = jnp.broadcast_to(flipped[:, 3:4], (LANES, LANES))
    across = iota((LANES, LANES), 1)
    spot = iota((32, LANES), 1)

    def right_side(r):
        here = spot + r * LANES
        pick = jnp.where(mine == here, 1.0, 0.0)
        stencil = -4.0 * pick
        stencil = stencil + jnp.where((mine == here - 1) & (spot != 0), 1.0, 0.0)
        stencil = stencil + jnp.where((mine == here + 1) & (spot != LANES - 1), 1.0, 0.0)
        stencil = stencil + jnp.where((mine == here - LANES) | (mine == here + LANES), 1.0, 0.0)
        stencil = stencil * on
        given = jnp.where(theirs == across + r * LANES, on_theirs, 0.0)
        return jnp.concatenate([pick, pick, stencil, stencil, given], 0).astype(jnp.bfloat16)

    right = [jnp.concatenate([right_side(r), right_side(r + 1)], 1) for r in range(0, ROWS, 2)]
    copies = []
    for n, first in enumerate(range(0, depth, CHUNK)):
        size = min(CHUNK, depth - first)
        part = left_side[first : first + size, :]
        for r in range(0, ROWS, 2):
            added = jnp.dot(part, right[r // 2], preferred_element_type=jnp.float32)
            for i in range(2):
                rows = pl.ds(first * ROWS + r + i, size, stride=ROWS)
                out_ref[rows, :] = inc_ref[rows, :] + added[:, i * LANES : (i + 1) * LANES]
        block = pl.ds(first * ROWS, size * ROWS)
        copies.append(pltpu.make_async_copy(out_ref.at[block], out_hbm.at[block], sems.at[n]))
        copies[-1].start()
    for copy in copies:
        copy.wait()


def swapped(x, axis, start, periodic):
    count = lax.axis_size(axis)
    pairs = []
    for i in range(start, count, 2):
        if periodic or i + 1 < count:
            pairs += [(i, (i + 1) % count), ((i + 1) % count, i)]
    return lax.ppermute(x, axis, pairs)


def on_device(increment, mixing, mixing_mask, jacobian, fp_col, fp_class, obs, obs_weight):
    f32 = jnp.float32
    peers = lax.axis_size("lat")
    depth = 2 * increment.shape[1]
    slots = fp_col.shape[2]
    kinds = jacobian.shape[0] * CH
    inc = increment.reshape(depth * ROWS, LANES)
    mix = mixing.reshape(depth, 1)
    jac = jnp.transpose(jacobian, (1, 0, 2)).reshape(kinds, depth)
    turned_jac = jnp.transpose(jac)
    struct = jax.ShapeDtypeStruct

    records = call(
        records_body, struct((peers, 1, SLOT * STRIDE), f32),
        (pltpu.VMEM((LANES, slots), f32), pltpu.VMEM((slots, LANES), f32), pltpu.VMEM((peers, SLOT * STRIDE), f32)),
        inputs=3, limit=None,
    )(obs.reshape(CH, 1, slots), obs_weight.reshape(CH, 1, slots), fp_class)
    records = lax.all_to_all(records, "lat", split_axis=0, concat_axis=0, tiled=True)

    edge = struct((depth, LANES), f32)
    edges = call(edges_body, (edge, edge, edge, edge))(inc)
    swaps = (("lon", 1, True), ("lat", 0, False), ("lat", 1, False), ("lon", 0, True))
    edges = [swapped(x, *swap) for x, swap in zip(edges, swaps)]

    seen, meta = call(
        state_body, (struct((kinds, LANES), f32), struct((8, LANES), f32)), inputs=9,
    )(inc, *edges, fp_col.reshape(1, slots), mixing_mask, mix, jac)
    own = call(
        departures_body, struct((32, LANES), f32),
        (pltpu.VMEM((8, SLOT * STRIDE), f32), pltpu.VMEM((LANES, LANES), f32)), inputs=3,
    )(records, seen, meta)

    out = call(
        gradient_body, struct((depth * ROWS, LANES), f32),
        (pltpu.VMEM((kinds, 2 * LANES), f32), pltpu.VMEM((LANES, LANES), f32),
         pltpu.VMEM((depth * ROWS, LANES), f32), pltpu.SemaphoreType.DMA((pl.cdiv(depth, CHUNK),))),
        inputs=8, space=pltpu.HBM,
    )(own, *(swapped(own, *swap) for swap in swaps[::-1]), turned_jac, mix, inc)
    return out.reshape(increment.shape)


def solution(mesh):
    return jax.shard_map(
        on_device,
        mesh=mesh,
        in_specs=(
            P(None, None, "lat", "lon"),
            P(),
            P("lat", "lon"),
            P(),
            P("lon", "lat", None),
            P("lon", "lat", None),
            P("lon", "lat", None, None),
            P("lon", "lat", None, None),
        ),
        out_specs=P(None, None, "lat", "lon"),
        check_vma=False,
    )
```

```python
import jax
import jax.numpy as jnp
from jax import lax
from jax.experimental import pallas as pl
from jax.experimental.pallas import tpu as pltpu
from jax.sharding import PartitionSpec as P

OWN_EVERY = 8
SLOT = 8
ROWS = 8
LANES = 128
STRIDE = 48
CH = 20
NOWHERE = -1000000
CHUNK = 112


def iota(shape, dim):
    return lax.broadcasted_iota(jnp.int32, shape, dim)


def call(body, out_shape, scratch=(), flops=1000000, inputs=1, limit=16 * 1024 * 1024, space=pltpu.VMEM):
    vmem = pl.BlockSpec(memory_space=pltpu.VMEM)
    return pl.pallas_call(
        body,
        out_shape=out_shape,
        in_specs=[vmem] * inputs,
        out_specs=jax.tree.map(lambda _: pl.BlockSpec(memory_space=space), out_shape),
        scratch_shapes=list(scratch),
        compiler_params=pltpu.CompilerParams(vmem_limit_bytes=limit),
        cost_estimate=pl.CostEstimate(flops=flops, bytes_accessed=1000000, transcendentals=0),
    )


def record_spots():
    return [((k * STRIDE) // LANES, (k * STRIDE) % LANES) for k in range(SLOT)]


def records_body(obs_ref, weight_ref, class_ref, out_ref, wide_ref, tall_ref, flat_ref):
    peers = out_ref.shape[0]
    wide_ref[...] = jnp.zeros(wide_ref.shape, jnp.float32)
    for ch in range(CH):
        wide_ref[ch : ch + 1, :] = obs_ref[ch]
        wide_ref[24 + ch : 25 + ch, :] = weight_ref[ch]
    wide_ref[CH : CH + 1, :] = class_ref[0].astype(jnp.float32)
    tall_ref[...] = jnp.transpose(wide_ref[...])
    lane = iota((peers, LANES), 1)
    tiles = [jnp.zeros((peers, LANES), jnp.float32) for _ in range(SLOT * STRIDE // LANES)]
    for k, (tile, off) in enumerate(record_spots()):
        part = tall_ref[pl.ds(k, peers, stride=SLOT), :]
        part = pltpu.roll(part, off, 1) if off else part
        if off + STRIDE <= LANES:
            tiles[tile] = tiles[tile] + part
        else:
            tiles[tile] = tiles[tile] + jnp.where(lane >= off, part, 0.0)
            tiles[tile + 1] = tiles[tile + 1] + jnp.where(lane < off, part, 0.0)
    for i, value in enumerate(tiles):
        flat_ref[:, i * LANES : (i + 1) * LANES] = value
    for s in range(peers):
        out_ref[s] = flat_ref[s : s + 1, :]


def is_even(axis):
    return lax.axis_index(axis) % 2 == 0


def edges_body(inc_ref, lon2_ref, lat_ref, lat2_ref, lon_ref):
    depth = lon_ref.shape[0]
    lane = iota((depth, LANES), 1)
    right = jnp.zeros((depth, LANES), jnp.float32)
    left = jnp.zeros((depth, LANES), jnp.float32)
    for r in range(ROWS):
        row = inc_ref[pl.ds(r, depth, stride=ROWS), :]
        if r == 0:
            first = row
        if r == ROWS - 1:
            last = row
        right = jnp.where(lane == r, pltpu.roll(row, r + 1, 1), right)
        left = jnp.where(lane == ROWS + r, pltpu.roll(row, ROWS + r, 1), left)
    even = is_even("lat")
    lat_ref[...] = jnp.where(even, last, first).astype(lat_ref.dtype)
    lat2_ref[...] = jnp.where(even, first, last).astype(lat2_ref.dtype)
    even = is_even("lon")
    lon_ref[...] = jnp.where(even, right, left).astype(lon_ref.dtype)
    lon2_ref[...] = jnp.where(even, left, right).astype(lon2_ref.dtype)


def state_body(inc_ref, lon2_ref, lat_ref, lat2_ref, lon_ref, col_ref, mask_ref, mix_ref,
               jac_ref, seen_ref, meta_ref):
    depth = lat_ref.shape[0]
    lane8 = iota((8, LANES), 1)
    cols = jnp.full((8, LANES), NOWHERE, jnp.int32)
    owners = col_ref.shape[1] // (SLOT * OWN_EVERY)
    for g in range(owners):
        start = g * SLOT * OWN_EVERY
        tile = jnp.broadcast_to(col_ref[:, start // LANES * LANES : start // LANES * LANES + LANES], (8, LANES))
        shift = (g * SLOT - start % LANES) % LANES
        tile = pltpu.roll(tile, shift, 1) if shift else tile
        cols = jnp.where((lane8 >= g * SLOT) & (lane8 < (g + 1) * SLOT), tile, cols)
    cols = jnp.where(cols >= 0, cols, NOWHERE)
    both = jnp.where(lane8 < 32, cols, jnp.where(lane8 < 64, pltpu.roll(cols, 32, 1), NOWHERE))
    want = jnp.broadcast_to(both[0:1, :], (LANES, LANES))
    sub = iota((LANES, LANES), 0)
    plain = iota((LANES, LANES), 1) < 32

    def split_dot(x, chosen):
        high = x.astype(jnp.bfloat16)
        low = (x - high.astype(jnp.float32)).astype(jnp.bfloat16)
        return jnp.dot(
            jnp.concatenate([high, low], 1), jnp.concatenate([chosen, chosen], 0),
            preferred_element_type=jnp.float32,
        )

    total = jnp.zeros((depth, LANES), jnp.float32)
    masked = jnp.zeros((8, LANES), jnp.float32)
    for r in range(ROWS):
        point = sub + r * LANES
        here = jnp.where(want == point, 1.0, 0.0)
        beside = jnp.where((want == point - 1) & (sub != 0), 1.0, 0.0)
        beside = beside + jnp.where((want == point + 1) & (sub != LANES - 1), 1.0, 0.0)
        beside = beside + jnp.where((want == point - LANES) | (want == point + LANES), 1.0, 0.0)
        chosen = jnp.where(plain, here, beside - 4.0 * here).astype(jnp.bfloat16)
        total = total + split_dot(inc_ref[pl.ds(r, depth, stride=ROWS), :], chosen)
        mask_row = jnp.broadcast_to(mask_ref[r : r + 1, :].astype(jnp.bfloat16), (8, LANES))
        masked = masked + jnp.dot(mask_row, chosen, preferred_element_type=jnp.float32)
    near = ~plain
    meets = jnp.where(is_even("lat"), (ROWS - 1) * LANES, 0)
    chosen = jnp.where(near & (want == sub + meets), 1.0, 0.0).astype(jnp.bfloat16)
    total = total + jnp.dot(lat_ref[...], chosen, preferred_element_type=jnp.float32)
    chosen = jnp.where(near & (want == sub + ((ROWS - 1) * LANES - meets)), 1.0, 0.0).astype(jnp.bfloat16)
    total = total + jnp.dot(lat2_ref[...], chosen, preferred_element_type=jnp.float32)
    on_left = (sub < ROWS) & (want == sub * LANES)
    on_right = (sub >= ROWS) & (sub < 2 * ROWS) & (want == (sub - ROWS) * LANES + LANES - 1)
    chosen = jnp.where(near & (on_left | on_right), 1.0, 0.0).astype(jnp.bfloat16)
    sides = lon_ref[...].astype(jnp.float32) + lon2_ref[...].astype(jnp.float32)
    total = total + jnp.dot(sides.astype(jnp.bfloat16), chosen, preferred_element_type=jnp.float32)

    state = total + mix_ref[...] * masked[0:1, :] * pltpu.roll(total, LANES - 32, 1)
    state = jnp.where(iota((depth, LANES), 1) < 32, state, 0.0).astype(jnp.bfloat16)
    seen_ref[...] = jnp.dot(jac_ref[...], state, preferred_element_type=jnp.float32)
    meta_ref[0:1, :] = cols[0:1, :].astype(jnp.float32)
    meta_ref[1:2, :] = masked[0:1, :]
    meta_ref[2:8, :] = jnp.zeros((6, LANES), jnp.float32)


def departures_body(records_ref, seen_ref, meta_ref, out_ref, row_ref, spot_ref):
    owners = records_ref.shape[0] // OWN_EVERY
    classes = seen_ref.shape[0] // CH
    row_ref[...] = jnp.zeros(row_ref.shape, jnp.float32)
    spot_ref[...] = jnp.zeros(spot_ref.shape, jnp.float32)
    for g in range(owners):
        row_ref[g : g + 1, :] = records_ref[g * OWN_EVERY]
    lane8 = iota((8, LANES), 1)
    tiles = [row_ref[:, i * LANES : (i + 1) * LANES] for i in range(SLOT * STRIDE // LANES)]
    for k, (tile, off) in enumerate(record_spots()):
        part = pltpu.roll(tiles[tile], LANES - off, 1) if off else tiles[tile]
        if off + STRIDE > LANES:
            part = jnp.where(lane8 < LANES - off, part, pltpu.roll(tiles[tile + 1], LANES - off, 1))
        for g in range(owners):
            spot_ref[g * SLOT + k : g * SLOT + k + 1, :] = part[g : g + 1, :]
    turned = jnp.transpose(spot_ref[...])
    lane1 = iota((1, LANES), 1)
    kind = jnp.where(lane1 < owners * SLOT, turned[CH : CH + 1, :], -1.0)
    chosen = jnp.broadcast_to(kind, (classes, LANES)).astype(jnp.int32) == iota((classes, LANES), 0)
    out_ref[...] = jnp.zeros(out_ref.shape, jnp.float32)
    for ch in range(CH):
        rows = seen_ref[ch * classes : (ch + 1) * classes, :]
        out_ref[ch : ch + 1, :] = jnp.sum(jnp.where(chosen, rows, 0.0), axis=0, keepdims=True)
    evolved = out_ref[0:CH, :]
    weighted = turned[24 : 24 + CH, :] * (evolved - turned[0:CH, :])
    weighted = jnp.where(jnp.broadcast_to(kind, (CH, LANES)) >= 0, weighted, 0.0)
    out_ref[0:CH, :] = weighted.astype(jnp.bfloat16).astype(jnp.float32)
    live = lane1 < owners * SLOT
    out_ref[CH : CH + 1, :] = jnp.where(live, kind, 0.0)
    out_ref[CH + 1 : CH + 2, :] = jnp.where(live, meta_ref[0:1, :], 0.0)
    out_ref[CH + 2 : CH + 3, :] = jnp.where(live, meta_ref[1:2, :], 0.0)
    col = meta_ref[0:1, :].astype(jnp.int32)
    across = col & (LANES - 1)
    ahead = [
        jnp.where(across == LANES - 1, col - (LANES - 1), NOWHERE),
        jnp.where(col >= (ROWS - 1) * LANES, col - (ROWS - 1) * LANES, NOWHERE),
    ]
    behind = [
        jnp.where(across == 0, col + (LANES - 1), NOWHERE),
        jnp.where((col >= 0) & (col < LANES), col + (ROWS - 1) * LANES, NOWHERE),
    ]
    for i, axis in enumerate(("lon", "lat")):
        even = is_even(axis)
        for j, swap in enumerate((even, jnp.logical_not(even))):
            spot = jnp.where(swap, ahead[i], behind[i]).astype(jnp.float32)
            row = CH + 3 + 2 * i + j
            out_ref[row : row + 1, :] = jnp.where(live, spot, 0.0)


def gradient_body(own_ref, lon_ref, lat2_ref, lat_ref, lon2_ref, turned_jac_ref, mix_ref, inc_ref,
                  out_hbm, spread_ref, flip_ref, out_ref, sems):
    depth = turned_jac_ref.shape[0]
    classes = turned_jac_ref.shape[1] // CH
    met = [ref[...] if i == 0 else pltpu.roll(ref[...], 32 * i, 1)
           for i, ref in enumerate((lon_ref, lon2_ref, lat_ref, lat2_ref))]
    others = met[0] + met[1] + met[2] + met[3]
    both = jnp.concatenate([own_ref[...], others], 1)
    kinds = jnp.broadcast_to(both[CH : CH + 1, :], (classes, 2 * LANES)).astype(jnp.int32)
    chosen = kinds == iota((classes, 2 * LANES), 0)
    for ch in range(CH):
        spread_ref[ch * classes : (ch + 1) * classes, :] = jnp.where(chosen, both[ch : ch + 1, :], 0.0)
    adjoint = jnp.dot(turned_jac_ref[...], spread_ref[...].astype(jnp.bfloat16), preferred_element_type=jnp.float32)

    own = jnp.where(iota((depth, LANES), 1) < 32, adjoint[:, 0:LANES], 0.0)
    own_high = own.astype(jnp.bfloat16).astype(jnp.float32)
    mixed = mix_ref[...] * own
    mixed_high = mixed.astype(jnp.bfloat16).astype(jnp.float32)
    parts = own_high + pltpu.roll(own - own_high, 32, 1)
    parts = parts + pltpu.roll(mixed_high, 64, 1) + pltpu.roll(mixed - mixed_high, 96, 1)
    left_side = jnp.concatenate([parts, mix_ref[...] * adjoint[:, LANES:]], 1).astype(jnp.bfloat16)

    flip_ref[...] = jnp.zeros(flip_ref.shape, jnp.float32)
    flip_ref[0:1, :] = own_ref[CH + 1 : CH + 2, :]
    flip_ref[1:2, :] = own_ref[CH + 2 : CH + 3, :]
    flip_ref[2:3, :] = sum(met[i][CH + 3 + n : CH + 4 + n, :] for i, n in enumerate((0, 1, 2, 3)))
    flip_ref[3:4, :] = others[CH + 2 : CH + 3, :]
    flipped = jnp.transpose(flip_ref[...])
    mine = jnp.broadcast_to(flipped[0:32, 0:1], (32, LANES)).astype(jnp.int32)
    on = jnp.broadcast_to(flipped[0:32, 1:2], (32, LANES))
    theirs = jnp.broadcast_to(flipped[:, 2:3], (LANES, LANES)).astype(jnp.int32)
    on_theirs = jnp.broadcast_to(flipped[:, 3:4], (LANES, LANES))
    across = iota((LANES, LANES), 1)
    spot = iota((32, LANES), 1)

    def right_side(r):
        here = spot + r * LANES
        pick = jnp.where(mine == here, 1.0, 0.0)
        stencil = -4.0 * pick
        stencil = stencil + jnp.where((mine == here - 1) & (spot != 0), 1.0, 0.0)
        stencil = stencil + jnp.where((mine == here + 1) & (spot != LANES - 1), 1.0, 0.0)
        stencil = stencil + jnp.where((mine == here - LANES) | (mine == here + LANES), 1.0, 0.0)
        stencil = stencil * on
        given = jnp.where(theirs == across + r * LANES, on_theirs, 0.0)
        return jnp.concatenate([pick, pick, stencil, stencil, given], 0).astype(jnp.bfloat16)

    right = [jnp.concatenate([right_side(r), right_side(r + 1)], 1) for r in range(0, ROWS, 2)]
    copies = []
    for n, first in enumerate(range(0, depth, CHUNK)):
        size = min(CHUNK, depth - first)
        part = left_side[first : first + size, :]
        for r in range(0, ROWS, 2):
            added = jnp.dot(part, right[r // 2], preferred_element_type=jnp.float32)
            for i in range(2):
                rows = pl.ds(first * ROWS + r + i, size, stride=ROWS)
                out_ref[rows, :] = inc_ref[rows, :] + added[:, i * LANES : (i + 1) * LANES]
        block = pl.ds(first * ROWS, size * ROWS)
        copies.append(pltpu.make_async_copy(out_ref.at[block], out_hbm.at[block], sems.at[n]))
        copies[-1].start()
    for copy in copies:
        copy.wait()


def swapped(x, axis, start, periodic):
    count = lax.axis_size(axis)
    pairs = []
    for i in range(start, count, 2):
        if periodic or i + 1 < count:
            pairs += [(i, (i + 1) % count), ((i + 1) % count, i)]
    return lax.ppermute(x, axis, pairs)


def on_device(increment, mixing, mixing_mask, jacobian, fp_col, fp_class, obs, obs_weight):
    f32 = jnp.float32
    peers = lax.axis_size("lat")
    depth = 2 * increment.shape[1]
    slots = fp_col.shape[2]
    kinds = jacobian.shape[0] * CH
    inc = increment.reshape(depth * ROWS, LANES)
    mix = mixing.reshape(depth, 1)
    jac = jnp.transpose(jacobian, (1, 0, 2)).reshape(kinds, depth)
    turned_jac = jnp.transpose(jac)
    struct = jax.ShapeDtypeStruct

    records = call(
        records_body, struct((peers, 1, SLOT * STRIDE), f32),
        (pltpu.VMEM((LANES, slots), f32), pltpu.VMEM((slots, LANES), f32), pltpu.VMEM((peers, SLOT * STRIDE), f32)),
        inputs=3, limit=None,
    )(obs.reshape(CH, 1, slots), obs_weight.reshape(CH, 1, slots), fp_class)
    records = lax.all_to_all(records, "lat", split_axis=0, concat_axis=0, tiled=True)

    edge = struct((depth, LANES), jnp.bfloat16)
    edges = call(edges_body, (edge, edge, edge, edge))(inc)
    swaps = (("lon", 1, True), ("lat", 0, False), ("lat", 1, False), ("lon", 0, True))
    edges = [swapped(x, *swap) for x, swap in zip(edges, swaps)]

    seen, meta = call(
        state_body, (struct((kinds, LANES), f32), struct((8, LANES), f32)), inputs=9,
    )(inc, *edges, fp_col.reshape(1, slots), mixing_mask, mix, jac)
    own = call(
        departures_body, struct((32, LANES), f32),
        (pltpu.VMEM((8, SLOT * STRIDE), f32), pltpu.VMEM((LANES, LANES), f32)), inputs=3,
    )(records, seen, meta)

    out = call(
        gradient_body, struct((depth * ROWS, LANES), f32),
        (pltpu.VMEM((kinds, 2 * LANES), f32), pltpu.VMEM((LANES, LANES), f32),
         pltpu.VMEM((depth * ROWS, LANES), f32), pltpu.SemaphoreType.DMA((pl.cdiv(depth, CHUNK),))),
        inputs=8, space=pltpu.HBM,
    )(own, *(swapped(own, *swap) for swap in swaps[::-1]), turned_jac, mix, inc)
    return out.reshape(increment.shape)


def solution(mesh):
    return jax.shard_map(
        on_device,
        mesh=mesh,
        in_specs=(
            P(None, None, "lat", "lon"),
            P(),
            P("lat", "lon"),
            P(),
            P("lon", "lat", None),
            P("lon", "lat", None),
            P("lon", "lat", None, None),
            P("lon", "lat", None, None),
        ),
        out_specs=P(None, None, "lat", "lon"),
        check_vma=False,
    )
```
